32 devices in a mesh: wide: 16 (over z, x, core), pair: 2 (over y).
Axes of the slice: x: 2, y: 2, z: 4, core: 2. Of those that a mesh axis runs over, the one named last changes fastest.
Arguments:
- pooled_b: bfloat16 [32, 16, 512, 128], P('wide', None, 'pair'), may hold values from -6 to 6
- dense_output_second: bfloat16 [8192, 128], P(('wide', 'pair')), may hold values from -4 to 4
- counts_b: int32 [8192, 26], P(('wide', 'pair')), may hold values from 1 to 8
- slot_of: int32 [32], replicated, may hold values from 0 to 31, each once
- stacked_a: bfloat16 [8192, 3456], P(('wide', 'pair')), may hold values from -4 to 4
- upstream_a: bfloat16 [8192, 3456], P(('wide', 'pair')), may hold values from -2 to 2
- counts_a: int32 [8192, 26], P(('wide', 'pair')), may hold values from 1 to 8
- down_projection: bfloat16 [3456, 512], P('wide'), may hold values from -0.109375 to 0.109375
- proj_up: bfloat16 [512, 3456], P(None, 'wide'), may hold values from -0.25 to 0.25
- cross_layer_bias: bfloat16 [3456], P('wide'), may hold values from -3 to 3
Outputs:
- crossed_b: bfloat16 [8192, 3456], P(('wide', 'pair'))
- dense_grad_a: bfloat16 [8192, 128], P(('wide', 'pair'))
- pooled_grad_a: bfloat16 [32, 16, 512, 128], P('wide', None, 'pair')
- grad_down: float32 [3456, 512], P('wide')
- grad_up: float32 [512, 3456], P(None, 'wide')
- grad_bias: float32 [3456], P('wide')
The draws below stay inside these ranges and needn't reach their ends.
Inputs may be any that keep to these rules, and one draw needn't show every extreme that they name: slot_of holds every slot once; its first 26 entries are the slots of tables 0 to 25, the rest are unused. Slot s lies on index s // 2 of wide.
All inputs are finite; a program needn't handle non-finite values.
Results may differ from the reference program's by a relative error of at most 0.0075.
Values may be sent and summed in bfloat16 or wider, within the bound.
A program may use at most 128 MiB of HBM per device.

```python
import jax
import jax.numpy as jnp
from jax import lax

E = 128
TABLES = 26
RANK = 512
SAMP = 256
POOL_MAX = 8
WIDTH = 3456
SLOTS = 32
BATCH = 8192
N_WIDE = 16
N_PAIR = 2


def touch_ends(drawn, stream_key, low, largest):
    dims = drawn.shape
    index_at = [jax.random.randint(jax.random.fold_in(stream_key, axis), (), 0, dims[axis]) for axis in range(len(dims))]
    drawn = drawn.at[tuple(index_at)].set(low)
    longest = dims.index(max(dims))
    index_at[longest] = (index_at[longest] + 1) % dims[longest]
    return drawn.at[tuple(index_at)].set(largest)


def raised(values, key, source, target, shards_of, factor):
    owner, partner = [(jnp.arange(values.shape[dim]) // (values.shape[dim] // shards_of)).reshape([-1 if axis == dim else 1 for axis in range(values.ndim)]) for dim in (source, target)]
    chosen = jax.random.permutation(key, shards_of)[partner]
    strong = (owner == chosen) | (owner == (partner + shards_of // 2) % shards_of)
    return jnp.where(strong, factor * values, values)


def block_scale(rng, extent, pieces, least, high):
    gain, own = 1.0, jax.random.fold_in(rng, 6)
    for axis_at, blocks in pieces:
        heights = jnp.exp(jax.random.uniform(jax.random.fold_in(own, axis_at), (blocks,), jnp.float32, least / len(pieces), high / len(pieces)))
        gain = gain * jnp.repeat(heights, extent[axis_at] // blocks).reshape([-1 if axis == axis_at else 1 for axis in range(len(extent))])
    return gain


def noise(rng, shape, spread, reach, split=(), kind=jnp.bfloat16):
    gain = block_scale(rng, shape, split, -0.22, 0.18) if split else 1.0
    drawn = jax.random.normal(rng, shape, jnp.float32) * spread * gain
    return jnp.minimum(jnp.maximum(drawn, -reach), reach).astype(kind)


def gaussian_with(key, dims, spread, limit, pieces, heavy, held_as=jnp.bfloat16):
    array = spread * jax.random.normal(key, dims, jnp.float32)
    if pieces:
        array = array * block_scale(key, dims, pieces, -0.22, 0.18)
    return jnp.clip(raised(array, jax.random.fold_in(key, 3), *heavy), -limit, limit).astype(held_as)


def setup_inputs(seed: int = 0) -> dict:
    keys = jax.random.split(jax.random.key(seed), 11)
    pooled_b = noise(keys[0], (SLOTS, N_WIDE, N_PAIR * SAMP, E), 1.0, 6.0, ((0, 16), (2, 2)))
    dense_output_second = noise(keys[1], (BATCH, E), 0.5, 4.0, ((0, 32),))
    counts_b = touch_ends(jax.random.randint(keys[2], (BATCH, TABLES), 1, POOL_MAX + 1), jax.random.fold_in(keys[2], 1), 1, POOL_MAX).astype(jnp.int32)
    slot_of = jax.random.permutation(keys[3], SLOTS).astype(jnp.int32)
    stacked_a = noise(keys[4], (BATCH, WIDTH), 0.5, 4.0, ((0, 32),))
    upstream_a = gaussian_with(keys[5], (BATCH, WIDTH), 0.25, 2.0, ((0, 32),), (0, 1, 32, 2.75))
    counts_a = touch_ends(jax.random.randint(keys[6], (BATCH, TABLES), 1, POOL_MAX + 1), jax.random.fold_in(keys[6], 1), 1, POOL_MAX).astype(jnp.int32)
    down_projection = noise(keys[7], (WIDTH, RANK), WIDTH ** -0.5, 0.109375, ((0, 16),))
    proj_up = noise(keys[8], (RANK, WIDTH), RANK ** -0.5, 0.25, ((1, 16),))
    cross_layer_bias = noise(keys[9], (WIDTH,), 0.5, 3.0, ((0, 16),))
    return {"pooled_b": pooled_b, "dense_output_second": dense_output_second, "counts_b": counts_b, "slot_of": slot_of, "stacked_a": stacked_a, "upstream_a": upstream_a, "counts_a": counts_a, "down_projection": down_projection, "proj_up": proj_up, "cross_layer_bias": cross_layer_bias}


def table_means(slot_rows, lookup_count, table_slots):
    picked = jnp.take(slot_rows, table_slots, axis=0).astype(jnp.float32)
    scaled = picked / jnp.transpose(lookup_count).astype(jnp.float32)[:, :, None]
    return jnp.transpose(scaled, (1, 0, 2)).reshape(scaled.shape[1], -1).astype(jnp.bfloat16)


def cross_forward(stacked, down, up):
    low_rank = jnp.dot(stacked, down, preferred_element_type=jnp.float32).astype(jnp.bfloat16)
    projected = jnp.dot(low_rank, up, preferred_element_type=jnp.float32)
    return low_rank, projected


def crossed_output(stacked, projected, bias):
    stacked_wide = stacked.astype(jnp.float32)
    return (stacked_wide * (projected + bias.astype(jnp.float32)) + stacked_wide).astype(jnp.bfloat16)


def cross_backward(stacked, upstream, lookup_count, down, up, bias, feature_index):
    low_rank, projected = cross_forward(stacked, down, up)
    stacked_wide = stacked.astype(jnp.float32)
    upstream_wide = upstream.astype(jnp.float32)
    scale_grad = upstream_wide * stacked_wide
    grad_bias = jnp.sum(scale_grad, axis=0)
    proj_grad = scale_grad.astype(jnp.bfloat16)
    over_rows = (((0,), (0,)), ((), ()))
    over_cols = (((1,), (1,)), ((), ()))
    grad_up = lax.dot_general(low_rank, proj_grad, over_rows, preferred_element_type=jnp.float32)
    low_grad = lax.dot_general(proj_grad, up, over_cols, preferred_element_type=jnp.float32).astype(jnp.bfloat16)
    grad_down = lax.dot_general(stacked, low_grad, over_rows, preferred_element_type=jnp.float32)
    input_grad = upstream_wide * (projected + bias.astype(jnp.float32)) + upstream_wide
    input_grad = input_grad + lax.dot_general(low_grad, down, over_cols, preferred_element_type=jnp.float32)
    rows = stacked.shape[0]
    dense_gradient = input_grad[:, :feature_index].astype(jnp.bfloat16)
    table_gradient = input_grad[:, feature_index:].reshape(rows, -1, feature_index) / lookup_count.astype(jnp.float32)[:, :, None]
    table_gradient = jnp.transpose(table_gradient, (1, 0, 2)).astype(jnp.bfloat16)
    return dense_gradient, table_gradient, grad_down, grad_up, grad_bias


def reference(pooled_b, dense_output_second, counts_b, slot_of, stacked_a, upstream_a, counts_a, down_projection, proj_up, cross_layer_bias):
    feature_index = dense_output_second.shape[1]
    table_slots = slot_of[:TABLES].astype(jnp.int32)
    slot_rows = pooled_b.reshape(SLOTS, BATCH, feature_index)

    def per_block(running, block_index):
        first_row = (block_index * SAMP).astype(jnp.int32)
        rows_b = lax.dynamic_slice_in_dim(slot_rows, first_row, SAMP, 1)
        dense_rows = lax.dynamic_slice_in_dim(dense_output_second, first_row, SAMP, 0)
        counts_rows_b = lax.dynamic_slice_in_dim(counts_b, first_row, SAMP, 0)
        stacked_b = jnp.concatenate([dense_rows, table_means(rows_b, counts_rows_b, table_slots)], axis=1)
        low_rank, projected = cross_forward(stacked_b, down_projection, proj_up)
        crossed = crossed_output(stacked_b, projected, cross_layer_bias)
        stacked_rows = lax.dynamic_slice_in_dim(stacked_a, first_row, SAMP, 0)
        upstream_rows = lax.dynamic_slice_in_dim(upstream_a, first_row, SAMP, 0)
        counts_rows_a = lax.dynamic_slice_in_dim(counts_a, first_row, SAMP, 0)
        dense_gradient, table_gradient, grad_d, grad_u, grad_b = cross_backward(
            stacked_rows, upstream_rows, counts_rows_a, down_projection, proj_up, cross_layer_bias, feature_index)
        slot_grad = jnp.zeros((SLOTS, SAMP, feature_index), jnp.bfloat16).at[table_slots].set(table_gradient)
        running = (running[0] + grad_d, running[1] + grad_u, running[2] + grad_b)
        return running, (crossed, dense_gradient, slot_grad)

    initial = (jnp.zeros((WIDTH, RANK), jnp.float32), jnp.zeros((RANK, WIDTH), jnp.float32),
               jnp.zeros((WIDTH,), jnp.float32))
    blocks = jnp.arange(BATCH // SAMP, dtype=jnp.int32)
    totals, (crossed, dense_gradient, slot_grad) = lax.scan(per_block, initial, blocks)
    crossed_b = crossed.reshape(BATCH, WIDTH)
    dense_grad_a = dense_gradient.reshape(BATCH, feature_index)
    pooled_grad_a = jnp.transpose(slot_grad, (1, 0, 2, 3)).reshape(SLOTS, N_WIDE, N_PAIR * SAMP, feature_index)
    return crossed_b, dense_grad_a, pooled_grad_a, totals[0], totals[1], totals[2]
```

```python
import functools

import jax
import jax.numpy as jnp
from jax import lax
from jax.experimental import pallas as pl
from jax.experimental.pallas import tpu as pltpu
from jax.sharding import PartitionSpec as P

MESH = pl.DeviceIdType.MESH


def flipped(index, mask):
    out = index
    bit = 1
    while bit <= mask:
        if mask & bit:
            out = out + bit - 2 * bit * lax.rem(index // bit, 2)
        bit *= 2
    return out


def stage_list(wide):
    stages = []
    mask = wide // 2
    while mask > 1:
        stages.append(("wide", mask))
        mask //= 2
    return stages + [("pair", 1), ("wide", 1)]


def meet(stages, partner):
    barrier = pltpu.get_barrier_semaphore()
    for stage in stages:
        pl.semaphore_signal(barrier, inc=1, device_id=partner(stage), device_id_type=MESH)
    pl.semaphore_wait(barrier, len(stages))


def gather_kernel(
    wide, down_ref, up_ref, vec_ref, down_out, up_out, vec_out,
    vec_held, vec_got, send_sem, recv_sem, local_sem, vec_send, vec_recv,
):
    me = lax.axis_index("wide")
    pair = lax.axis_index("pair")
    stages = stage_list(wide)
    half = down_ref.shape[1] // 2
    starts = (pl.multiple_of(pair * half, half), pl.multiple_of((1 - pair) * half, half))
    ins, outs = (down_ref, up_ref), (down_out, up_out)

    def partner(stage):
        if stage[0] == "pair":
            return {"pair": 1 - pair}
        return {"wide": flipped(me, stage[1])}

    meet(stages, partner)
    sends = []

    def copy(stage, source, part, kind, received, which):
        columns = pl.ds(starts[part], half)
        block = flipped(me, source)
        if source == 0:
            src = ins[kind].at[:, columns]
        else:
            src = outs[kind].at[block, :, columns]
        return pltpu.make_async_remote_copy(
            src_ref=src,
            dst_ref=outs[kind].at[block, :, columns],
            send_sem=send_sem.at[which],
            recv_sem=recv_sem.at[received],
            device_id=partner(stage),
            device_id_type=MESH,
        )

    def slot(offset, part, kind):
        return (offset * 2 + part) * 2 + kind

    def forward(position, source, part):
        for stage in stages[position:]:
            if stage[0] == "pair":
                if part == 1 or source == 0:
                    continue
                offset, got_part = source, 1
            else:
                offset, got_part = source ^ stage[1], part
            for kind in range(2):
                made = copy(stage, source, part, kind, slot(offset, got_part, kind), len(sends))
                made.start()
                sends.append(made)

    def await_block(offset, part):
        columns = pl.ds(starts[part], half)
        block = flipped(me, offset)
        for kind in range(2):
            view = outs[kind].at[block, :, columns]
            pltpu.make_async_copy(view, view, recv_sem.at[slot(offset, part, kind)]).wait()

    def vector(index, stage):
        return pltpu.make_async_remote_copy(
            src_ref=vec_held.at[index],
            dst_ref=vec_got.at[index],
            send_sem=vec_send.at[index],
            recv_sem=vec_recv.at[index],
            device_id=partner(stage),
            device_id_type=MESH,
        )

    vec_held[0] = vec_ref[...]
    vectors = [vector(index, stage) for index, stage in enumerate(stages)]
    forward(0, 0, 0)
    forward(len(stages) - 1, 0, 1)
    vectors[0].start()
    own = []
    for kind in range(2):
        keep = pltpu.make_async_copy(ins[kind], outs[kind].at[me], local_sem.at[kind])
        keep.start()
        own.append(keep)

    known = [0]
    for position, stage in enumerate(stages):
        if stage[0] == "pair":
            for offset in known[1:]:
                await_block(offset, 1)
                forward(position + 1, offset, 1)
        elif stage[1] > 1:
            arrived = [offset ^ stage[1] for offset in known]
            for offset in arrived:
                await_block(offset, 0)
                forward(position + 1, offset, 0)
            known = known + arrived
        else:
            for offset in known:
                for part in range(2):
                    await_block(offset ^ 1, part)
        vectors[position].wait_recv()
        total = vec_held[position] + vec_got[position]
        if position + 1 < len(stages):
            vec_held[position + 1] = total
            vectors[position + 1].start()
        else:
            vec_out[...] = total
    for keep in own:
        keep.wait()
    for made in sends + vectors:
        made.wait_send()


def gathered(wide, down, up, vec, collective_id=0):
    rows, rank = down.shape
    count = len(stage_list(wide))
    trees = 2 * (wide // 2 - 1 + wide // 2 - 1 + wide)
    vmem = pl.BlockSpec(memory_space=pltpu.VMEM)
    hbm = pl.BlockSpec(memory_space=pl.ANY)
    return pl.pallas_call(
        functools.partial(gather_kernel, wide),
        out_shape=(
            jax.ShapeDtypeStruct((wide, rows, rank), down.dtype),
            jax.ShapeDtypeStruct((wide, rows, rank), up.dtype),
            jax.ShapeDtypeStruct(vec.shape, vec.dtype),
        ),
        in_specs=[vmem, vmem, vmem],
        out_specs=(hbm, hbm, vmem),
        scratch_shapes=[
            pltpu.VMEM((count,) + vec.shape, vec.dtype),
            pltpu.VMEM((count,) + vec.shape, vec.dtype),
            pltpu.SemaphoreType.DMA((trees,)),
            pltpu.SemaphoreType.DMA((4 * wide,)),
            pltpu.SemaphoreType.DMA((2,)),
            pltpu.SemaphoreType.DMA((count,)),
            pltpu.SemaphoreType.DMA((count,)),
        ],
        compiler_params=pltpu.CompilerParams(
            collective_id=collective_id, has_side_effects=True
        ),
        cost_estimate=pl.CostEstimate(
            flops=0, bytes_accessed=wide * rows * rank * 40, transcendentals=0
        ),
        name="weights_gather",
    )(down, up, vec)


def tree_slots(wide):
    slots = {}
    mask = 2
    while mask < wide:
        for offset in range(0, wide, 2 * mask):
            slots[(mask, offset)] = len(slots)
        mask *= 2
    return slots


def scatter_kernel(
    wide, down_ref, up_ref, down_out, up_out,
    core_got, pair_send, pair_got, tree_send, tree_got, last_send, last_got,
    core_sems, pair_sems, tree_sems, last_sems,
):
    me = lax.axis_index("wide")
    pair = lax.axis_index("pair")
    stages = stage_list(wide)
    slots = tree_slots(wide)
    half = down_ref.shape[2] // 2
    mine = pl.ds(pl.multiple_of(pair * half, half), half)
    other = pl.ds(pl.multiple_of((1 - pair) * half, half), half)
    ins, outs = (down_ref, up_ref), (down_out, up_out)
    evens = list(range(0, wide, 2))
    bits = wide.bit_length()
    order = sorted(
        evens, key=lambda e: [(e >> b) & 1 for b in range(1, bits)], reverse=True
    )

    def partner(stage):
        if stage[0] == "pair":
            return {"pair": 1 - pair}
        return {"wide": flipped(me, stage[1])}

    meet(stages, partner)

    def remote(src, dst, sems, index, stage):
        return pltpu.make_async_remote_copy(
            src_ref=src,
            dst_ref=dst,
            send_sem=sems.at[0, index],
            recv_sem=sems.at[1, index],
            device_id=partner(stage),
            device_id_type=MESH,
        )

    core_copies = {}
    for part, columns in ((1, other), (0, mine)):
        for offset in order:
            for kind in range(2):
                made = remote(
                    ins[kind].at[flipped(me, offset ^ 1), :, columns],
                    core_got.at[kind, offset // 2, :, columns],
                    core_sems,
                    (offset // 2 * 2 + part) * 2 + kind,
                    ("wide", 1),
                )
                made.start()
                core_copies[(part, offset, kind)] = made

    def both_cores(kind, offset, columns):
        own = ins[kind][flipped(me, offset), :, columns].astype(jnp.float32)
        return own + core_got[kind, offset // 2, :, columns].astype(jnp.float32)

    pair_copies = {}
    for offset in order:
        for kind in range(2):
            core_copies[(1, offset, kind)].wait_recv()
            pair_send[kind, offset // 2] = both_cores(kind, offset, other).astype(jnp.bfloat16)
            made = remote(
                pair_send.at[kind, offset // 2],
                pair_got.at[kind, offset // 2],
                pair_sems,
                offset // 2 * 2 + kind,
                ("pair", 1),
            )
            made.start()
            pair_copies[(offset, kind)] = made

    tree_copies = []
    last_copies = []
    for offset in order:
        for kind in range(2):
            core_copies[(0, offset, kind)].wait_recv()
            pair_copies[(offset, kind)].wait_recv()
            total = both_cores(kind, offset, mine)
            total = total + pair_got[kind, offset // 2].astype(jnp.float32)
            mask = 2
            while mask < wide and not offset & mask:
                index = slots[(mask, offset)]
                view = tree_got.at[kind, index]
                pltpu.make_async_copy(view, view, tree_sems.at[1, index * 2 + kind]).wait()
                total = total + tree_got[kind, index].astype(jnp.float32)
                mask *= 2
            if mask < wide:
                index = slots[(mask, offset ^ mask)]
                tree_send[kind, index] = total.astype(jnp.bfloat16)
                made = remote(
                    tree_send.at[kind, index],
                    tree_got.at[kind, index],
                    tree_sems,
                    index * 2 + kind,
                    ("wide", mask),
                )
                made.start()
                tree_copies.append(made)
            else:
                rounded = total.astype(jnp.bfloat16)
                last_send[kind] = rounded
                made = remote(
                    last_send.at[kind], last_got.at[kind], last_sems, kind, ("pair", 1)
                )
                made.start()
                last_copies.append(made)
                outs[kind][:, mine] = rounded.astype(jnp.float32)
    for kind in range(2):
        last_copies[kind].wait_recv()
        outs[kind][:, other] = last_got[kind].astype(jnp.float32)
    for made in list(core_copies.values()) + list(pair_copies.values()):
        made.wait_send()
    for made in tree_copies + last_copies:
        made.wait_send()


def scattered(wide, grad_down, grad_up, collective_id=1):
    _, rows, rank = grad_down.shape
    half = rank // 2
    slots = len(tree_slots(wide))
    vmem = pl.BlockSpec(memory_space=pltpu.VMEM)
    held = jnp.bfloat16
    return pl.pallas_call(
        functools.partial(scatter_kernel, wide),
        out_shape=(
            jax.ShapeDtypeStruct((rows, rank), jnp.float32),
            jax.ShapeDtypeStruct((rows, rank), jnp.float32),
        ),
        in_specs=[vmem, vmem],
        out_specs=(vmem, vmem),
        scratch_shapes=[
            pltpu.VMEM((2, wide // 2, rows, rank), held),
            pltpu.VMEM((2, wide // 2, rows, half), held),
            pltpu.VMEM((2, wide // 2, rows, half), held),
            pltpu.VMEM((2, slots, rows, half), held),
            pltpu.VMEM((2, slots, rows, half), held),
            pltpu.VMEM((2, rows, half), held),
            pltpu.VMEM((2, rows, half), held),
            pltpu.SemaphoreType.DMA((2, 2 * wide)),
            pltpu.SemaphoreType.DMA((2, wide)),
            pltpu.SemaphoreType.DMA((2, 2 * slots)),
            pltpu.SemaphoreType.DMA((2, 2)),
        ],
        compiler_params=pltpu.CompilerParams(
            collective_id=collective_id, has_side_effects=True,
            vmem_limit_bytes=40 * 1024 * 1024,
        ),
        cost_estimate=pl.CostEstimate(
            flops=0, bytes_accessed=wide * rows * rank * 40, transcendentals=0
        ),
        name="gradients_scatter",
    )(grad_down, grad_up)


def table_means(slot_rows, lookup_count, table_slots):
    picked = jnp.take(slot_rows, table_slots, axis=0).astype(jnp.float32)
    scaled = picked / jnp.transpose(lookup_count).astype(jnp.float32)[:, :, None]
    return jnp.transpose(scaled, (1, 0, 2)).reshape(scaled.shape[1], -1).astype(jnp.bfloat16)


OVER_ROWS = (((0,), (0,)), ((), ()))
OVER_COLS = (((1,), (1,)), ((), ()))


def dot(left, right, dims):
    return lax.dot_general(left, right, dims, preferred_element_type=jnp.float32)


def cross_forward(stacked, down, up_rows):
    low_rank = jnp.dot(stacked, down, preferred_element_type=jnp.float32).astype(jnp.bfloat16)
    return low_rank, dot(low_rank, up_rows, OVER_COLS)


def local(
    wide,
    pooled_b,
    dense_output_second,
    counts_b,
    slot_of,
    stacked_a,
    upstream_a,
    counts_a,
    down_projection,
    proj_up,
    cross_layer_bias,
):
    feature = dense_output_second.shape[1]
    tables = counts_b.shape[1]
    table_slots = slot_of[:tables]
    shard = down_projection.shape[0]
    rank = down_projection.shape[1]
    width = stacked_a.shape[1]
    samples = stacked_a.shape[0]
    me = lax.axis_index("wide")
    lanes = -(-shard // 128) * 128

    stacked_wide = stacked_a.astype(jnp.float32)
    upstream_wide = upstream_a.astype(jnp.float32)
    scale_grad = upstream_wide * stacked_wide
    bias_share = jnp.sum(scale_grad, axis=0).reshape(wide, shard)
    holds = (jnp.arange(wide) == me) & (lax.axis_index("pair") == 0)
    bias_own = jnp.where(holds[:, None], cross_layer_bias.astype(jnp.float32)[None, :], 0.0)
    vec = jnp.pad(jnp.concatenate([bias_share, bias_own], axis=0), ((0, 0), (0, lanes - shard)))
    down_all, up_all, vec_all = gathered(wide, down_projection, jnp.transpose(proj_up), vec)
    grad_bias = lax.dynamic_index_in_dim(vec_all, me, 0, keepdims=False)[:shard]
    bias = vec_all[wide:, :shard].reshape(width)

    pooled_b, down_all = lax.optimization_barrier((pooled_b, down_all))
    arrived = lax.all_to_all(pooled_b, "wide", split_axis=1, concat_axis=0, tiled=True)
    slot_count = arrived.shape[0]

    down = down_all.reshape(width, rank)
    up_rows = up_all.reshape(width, rank)

    proj_grad = scale_grad.astype(jnp.bfloat16)
    low_grad = jnp.dot(proj_grad, up_rows, preferred_element_type=jnp.float32).astype(jnp.bfloat16)
    low_a, projected = cross_forward(stacked_a, down, up_rows)
    input_grad = upstream_wide * (projected + bias) + upstream_wide
    input_grad = input_grad + dot(low_grad, down, OVER_COLS)
    grad_down = dot(stacked_a, low_grad, OVER_ROWS).astype(jnp.bfloat16)
    grad_up = dot(proj_grad, low_a, OVER_ROWS).astype(jnp.bfloat16)
    dense_gradient = input_grad[:, :feature].astype(jnp.bfloat16)
    table_gradient = (
        input_grad[:, feature:].reshape(samples, -1, feature)
        / counts_a.astype(jnp.float32)[:, :, None]
    )
    table_gradient = jnp.transpose(table_gradient, (1, 0, 2)).astype(jnp.bfloat16)
    slot_selector = (
        table_slots[None, :] == jnp.arange(slot_count, dtype=jnp.int32)[:, None]
    ).astype(jnp.bfloat16)
    slot_grad = jnp.einsum(
        "qv,vxk->qxk", slot_selector, table_gradient, preferred_element_type=jnp.float32
    ).astype(jnp.bfloat16)
    slot_grad, grad_down, grad_up = lax.optimization_barrier((slot_grad, grad_down, grad_up))
    returned = lax.all_to_all(
        slot_grad.reshape(slot_count, 1, samples, feature),
        "wide",
        split_axis=0,
        concat_axis=1,
        tiled=True,
    )
    down_sum, up_sum = scattered(
        wide, grad_down.reshape(wide, shard, rank), grad_up.reshape(wide, shard, rank)
    )

    slot_rows = arrived.reshape(slot_count, samples, feature)
    stacked_b = jnp.concatenate(
        [dense_output_second, table_means(slot_rows, counts_b, table_slots)], axis=1
    )
    _, projected_b = cross_forward(stacked_b, down, up_rows)
    b_wide = stacked_b.astype(jnp.float32)
    crossed_b = (b_wide * (projected_b + bias) + b_wide).astype(jnp.bfloat16)
    return (crossed_b, dense_gradient, returned, down_sum, jnp.transpose(up_sum), grad_bias)


def solution(mesh):
    return jax.shard_map(
        functools.partial(local, mesh.shape["wide"]),
        mesh=mesh,
        in_specs=(
            P("wide", None, "pair", None),
            P(("wide", "pair"), None),
            P(("wide", "pair"), None),
            P(),
            P(("wide", "pair"), None),
            P(("wide", "pair"), None),
            P(("wide", "pair"), None),
            P("wide", None),
            P(None, "wide"),
            P("wide"),
        ),
        out_specs=(
            P(("wide", "pair"), None),
            P(("wide", "pair"), None),
            P("wide", None, "pair", None),
            P("wide", None),
            P(None, "wide"),
            P("wide"),
        ),
        check_vma=False,
    )
```

```python
import functools

import jax
import jax.numpy as jnp
from jax import lax
from jax.experimental import pallas as pl
from jax.experimental.pallas import tpu as pltpu
from jax.sharding import PartitionSpec as P

MESH = pl.DeviceIdType.MESH


def flipped(index, mask):
    out = index
    bit = 1
    while bit <= mask:
        if mask & bit:
            out = out + bit - 2 * bit * lax.rem(index // bit, 2)
        bit *= 2
    return out


def stage_list(wide):
    stages = []
    mask = wide // 2
    while mask > 1:
        stages.append(("wide", mask))
        mask //= 2
    return stages + [("pair", 1), ("wide", 1)]


def meet(wide, me, pair):
    barrier = pltpu.get_barrier_semaphore()
    for offset in range(1, wide):
        pl.semaphore_signal(
            barrier, inc=1, device_id={"wide": flipped(me, offset)}, device_id_type=MESH
        )
    pl.semaphore_signal(barrier, inc=1, device_id={"pair": 1 - pair}, device_id_type=MESH)
    pl.semaphore_wait(barrier, wide)


def exchange(wide, me, source, target, sems):
    copies = []
    for offset in range(wide - 1, 0, -1):
        peer = flipped(me, offset)
        made = pltpu.make_async_remote_copy(
            src_ref=source(peer),
            dst_ref=target(me),
            send_sem=sems.at[0, offset],
            recv_sem=sems.at[1, offset],
            device_id={"wide": peer},
            device_id_type=MESH,
        )
        made.start()
        copies.append(made)
    keep = pltpu.make_async_copy(source(me), target(me), sems.at[0, 0])
    keep.start()
    return copies, keep


def gather_kernel(
    wide, down_ref, up_ref, vec_ref, pooled_ref, down_out, up_out, vec_out, arrived_out,
    vec_held, vec_got, send_sem, recv_sem, local_sem, vec_send, vec_recv, swap_sems,
):
    me = lax.axis_index("wide")
    pair = lax.axis_index("pair")
    stages = stage_list(wide)
    half = down_ref.shape[1] // 2
    starts = (pl.multiple_of(pair * half, half), pl.multiple_of((1 - pair) * half, half))
    ins, outs = (down_ref, up_ref), (down_out, up_out)

    def partner(stage):
        if stage[0] == "pair":
            return {"pair": 1 - pair}
        return {"wide": flipped(me, stage[1])}

    meet(wide, me, pair)
    sends = []

    def copy(stage, source, part, kind, received, which):
        columns = pl.ds(starts[part], half)
        block = flipped(me, source)
        if source == 0:
            src = ins[kind].at[:, columns]
        else:
            src = outs[kind].at[block, :, columns]
        return pltpu.make_async_remote_copy(
            src_ref=src,
            dst_ref=outs[kind].at[block, :, columns],
            send_sem=send_sem.at[which],
            recv_sem=recv_sem.at[received],
            device_id=partner(stage),
            device_id_type=MESH,
        )

    def slot(offset, part, kind):
        return (offset * 2 + part) * 2 + kind

    def forward(position, source, part):
        for stage in stages[position:]:
            if stage[0] == "pair":
                if part == 1 or source == 0:
                    continue
                offset, got_part = source, 1
            else:
                offset, got_part = source ^ stage[1], part
            for kind in range(2):
                made = copy(stage, source, part, kind, slot(offset, got_part, kind), len(sends))
                made.start()
                sends.append(made)

    def await_block(offset, part):
        columns = pl.ds(starts[part], half)
        block = flipped(me, offset)
        for kind in range(2):
            view = outs[kind].at[block, :, columns]
            pltpu.make_async_copy(view, view, recv_sem.at[slot(offset, part, kind)]).wait()

    def vector(index, stage):
        return pltpu.make_async_remote_copy(
            src_ref=vec_held.at[index],
            dst_ref=vec_got.at[index],
            send_sem=vec_send.at[index],
            recv_sem=vec_recv.at[index],
            device_id=partner(stage),
            device_id_type=MESH,
        )

    vec_held[0] = vec_ref[...]
    vectors = [vector(index, stage) for index, stage in enumerate(stages)]
    forward(0, 0, 0)
    forward(len(stages) - 1, 0, 1)
    vectors[0].start()
    own = []
    for kind in range(2):
        keep = pltpu.make_async_copy(ins[kind], outs[kind].at[me], local_sem.at[kind])
        keep.start()
        own.append(keep)

    each = pooled_ref.shape[0]
    swaps = None
    known = [0]
    for position, stage in enumerate(stages):
        if swaps is None and (stage[0] == "pair" or stage[1] == 2):
            swaps, stay = exchange(
                wide,
                me,
                lambda peer: pooled_ref.at[:, peer],
                lambda owner: arrived_out.at[pl.ds(owner * each, each)],
                swap_sems,
            )
        if stage[0] == "pair":
            for offset in known[1:]:
                await_block(offset, 1)
                forward(position + 1, offset, 1)
        elif stage[1] > 1:
            arrived = [offset ^ stage[1] for offset in known]
            for offset in arrived:
                await_block(offset, 0)
                forward(position + 1, offset, 0)
            known = known + arrived
        else:
            for offset in known:
                for part in range(2):
                    await_block(offset ^ 1, part)
        vectors[position].wait_recv()
        total = vec_held[position] + vec_got[position]
        if position + 1 < len(stages):
            vec_held[position + 1] = total
            vectors[position + 1].start()
        else:
            vec_out[...] = total
    for keep in own + [stay]:
        keep.wait()
    for made in swaps:
        made.wait()
    for made in sends + vectors:
        made.wait_send()


def gathered(wide, down, up, vec, pooled, collective_id=0):
    rows, rank = down.shape
    count = len(stage_list(wide))
    trees = 2 * (wide // 2 - 1 + wide // 2 - 1 + wide)
    vmem = pl.BlockSpec(memory_space=pltpu.VMEM)
    hbm = pl.BlockSpec(memory_space=pl.ANY)
    return pl.pallas_call(
        functools.partial(gather_kernel, wide),
        out_shape=(
            jax.ShapeDtypeStruct((wide, rows, rank), down.dtype),
            jax.ShapeDtypeStruct((wide, rows, rank), up.dtype),
            jax.ShapeDtypeStruct(vec.shape, vec.dtype),
            jax.ShapeDtypeStruct((pooled.shape[0] * wide,) + pooled.shape[2:], pooled.dtype),
        ),
        in_specs=[vmem, vmem, vmem, hbm],
        out_specs=(hbm, hbm, vmem, hbm),
        scratch_shapes=[
            pltpu.VMEM((count,) + vec.shape, vec.dtype),
            pltpu.VMEM((count,) + vec.shape, vec.dtype),
            pltpu.SemaphoreType.DMA((trees,)),
            pltpu.SemaphoreType.DMA((4 * wide,)),
            pltpu.SemaphoreType.DMA((2,)),
            pltpu.SemaphoreType.DMA((count,)),
            pltpu.SemaphoreType.DMA((count,)),
            pltpu.SemaphoreType.DMA((2, wide)),
        ],
        compiler_params=pltpu.CompilerParams(
            collective_id=collective_id, has_side_effects=True
        ),
        cost_estimate=pl.CostEstimate(
            flops=0, bytes_accessed=wide * rows * rank * 40, transcendentals=0
        ),
        name="weights_gather",
    )(down, up, vec, pooled)


def tree_slots(wide):
    slots = {}
    mask = 2
    while mask < wide:
        for offset in range(0, wide, 2 * mask):
            slots[(mask, offset)] = len(slots)
        mask *= 2
    return slots


def scatter_kernel(
    wide, down_ref, up_ref, slot_grad_ref, slot_ref, arrived_ref, dense_ref, counts_ref,
    weight_down_ref, weight_up_ref, bias_ref,
    down_out, up_out, returned_out, crossed_out,
    stacked_held, low_held, core_got, pair_send, pair_got, tree_send, tree_got, last_send, last_got,
    core_sems, pair_sems, tree_sems, last_sems, swap_sems,
):
    me = lax.axis_index("wide")
    pair = lax.axis_index("pair")
    stages = stage_list(wide)
    slots = tree_slots(wide)
    half = down_ref.shape[2] // 2
    mine = pl.ds(pl.multiple_of(pair * half, half), half)
    other = pl.ds(pl.multiple_of((1 - pair) * half, half), half)
    ins, outs = (down_ref, up_ref), (down_out, up_out)
    evens = list(range(0, wide, 2))
    bits = wide.bit_length()
    order = sorted(
        evens, key=lambda e: [(e >> b) & 1 for b in range(1, bits)], reverse=True
    )

    def partner(stage):
        if stage[0] == "pair":
            return {"pair": 1 - pair}
        return {"wide": flipped(me, stage[1])}

    meet(wide, me, pair)

    def remote(src, dst, sems, index, stage):
        return pltpu.make_async_remote_copy(
            src_ref=src,
            dst_ref=dst,
            send_sem=sems.at[0, index],
            recv_sem=sems.at[1, index],
            device_id=partner(stage),
            device_id_type=MESH,
        )

    core_copies = {}
    for part, columns in ((1, other), (0, mine)):
        for offset in order:
            for kind in range(2):
                made = remote(
                    ins[kind].at[flipped(me, offset ^ 1), :, columns],
                    core_got.at[kind, offset // 2, :, columns],
                    core_sems,
                    (offset // 2 * 2 + part) * 2 + kind,
                    ("wide", 1),
                )
                made.start()
                core_copies[(part, offset, kind)] = made

    each = returned_out.shape[0]
    swaps, stay = exchange(
        wide,
        me,
        lambda peer: slot_grad_ref.at[pl.ds(peer * each, each)],
        lambda owner: returned_out.at[:, owner],
        swap_sems,
    )

    def both_cores(kind, offset, columns):
        own = ins[kind][flipped(me, offset), :, columns].astype(jnp.float32)
        return own + core_got[kind, offset // 2, :, columns].astype(jnp.float32)

    pair_copies = {}
    for offset in order:
        for kind in range(2):
            core_copies[(1, offset, kind)].wait_recv()
            pair_send[kind, offset // 2] = both_cores(kind, offset, other).astype(jnp.bfloat16)
            made = remote(
                pair_send.at[kind, offset // 2],
                pair_got.at[kind, offset // 2],
                pair_sems,
                offset // 2 * 2 + kind,
                ("pair", 1),
            )
            made.start()
            pair_copies[(offset, kind)] = made

    forward_b(
        slot_ref, arrived_ref, dense_ref, counts_ref, weight_down_ref, weight_up_ref, bias_ref,
        crossed_out, stacked_held, low_held,
    )

    tree_copies = []
    last_copies = []
    for offset in order:
        for kind in range(2):
            core_copies[(0, offset, kind)].wait_recv()
            pair_copies[(offset, kind)].wait_recv()
            total = both_cores(kind, offset, mine)
            total = total + pair_got[kind, offset // 2].astype(jnp.float32)
            mask = 2
            while mask < wide and not offset & mask:
                index = slots[(mask, offset)]
                view = tree_got.at[kind, index]
                pltpu.make_async_copy(view, view, tree_sems.at[1, index * 2 + kind]).wait()
                total = total + tree_got[kind, index].astype(jnp.float32)
                mask *= 2
            if mask < wide:
                index = slots[(mask, offset ^ mask)]
                tree_send[kind, index] = total.astype(jnp.bfloat16)
                made = remote(
                    tree_send.at[kind, index],
                    tree_got.at[kind, index],
                    tree_sems,
                    index * 2 + kind,
                    ("wide", mask),
                )
                made.start()
                tree_copies.append(made)
            else:
                rounded = total.astype(jnp.bfloat16)
                last_send[kind] = rounded
                made = remote(
                    last_send.at[kind], last_got.at[kind], last_sems, kind, ("pair", 1)
                )
                made.start()
                last_copies.append(made)
                outs[kind][:, mine] = rounded.astype(jnp.float32)
    for kind in range(2):
        last_copies[kind].wait_recv()
        outs[kind][:, other] = last_got[kind].astype(jnp.float32)
    for made in list(core_copies.values()) + list(pair_copies.values()):
        made.wait_send()
    for made in tree_copies + last_copies:
        made.wait_send()
    for made in swaps:
        made.wait()
    stay.wait()


def scattered(wide, grad_down, grad_up, slot_grad, forward, collective_id=1):
    _, rows, rank = grad_down.shape
    half = rank // 2
    slots = len(tree_slots(wide))
    vmem = pl.BlockSpec(memory_space=pltpu.VMEM)
    hbm = pl.BlockSpec(memory_space=pl.ANY)
    held = jnp.bfloat16
    slots_all, samples = slot_grad.shape[:2]
    return pl.pallas_call(
        functools.partial(scatter_kernel, wide),
        out_shape=(
            jax.ShapeDtypeStruct((rows, rank), jnp.float32),
            jax.ShapeDtypeStruct((rows, rank), jnp.float32),
            jax.ShapeDtypeStruct((slots_all // wide, wide) + slot_grad.shape[1:], held),
            jax.ShapeDtypeStruct((samples, wide * rows), held),
        ),
        in_specs=[vmem, vmem, hbm, pl.BlockSpec(memory_space=pltpu.SMEM)] + [vmem] * 6,
        out_specs=(vmem, vmem, hbm, vmem),
        scratch_shapes=[
            pltpu.VMEM((samples, wide * rows), held),
            pltpu.VMEM((samples, rank), jnp.float32),
            pltpu.VMEM((2, wide // 2, rows, rank), held),
            pltpu.VMEM((2, wide // 2, rows, half), held),
            pltpu.VMEM((2, wide // 2, rows, half), held),
            pltpu.VMEM((2, slots, rows, half), held),
            pltpu.VMEM((2, slots, rows, half), held),
            pltpu.VMEM((2, rows, half), held),
            pltpu.VMEM((2, rows, half), held),
            pltpu.SemaphoreType.DMA((2, 2 * wide)),
            pltpu.SemaphoreType.DMA((2, wide)),
            pltpu.SemaphoreType.DMA((2, 2 * slots)),
            pltpu.SemaphoreType.DMA((2, 2)),
            pltpu.SemaphoreType.DMA((2, wide)),
        ],
        compiler_params=pltpu.CompilerParams(
            collective_id=collective_id, has_side_effects=True,
            vmem_limit_bytes=VMEM_LIMIT,
        ),
        cost_estimate=pl.CostEstimate(
            flops=0, bytes_accessed=wide * rows * rank * 40, transcendentals=0
        ),
        name="gradients_scatter",
    )(grad_down, grad_up, slot_grad, *forward)


OVER_ROWS = (((0,), (0,)), ((), ()))
OVER_COLS = (((1,), (1,)), ((), ()))
PLAIN = (((1,), (0,)), ((), ()))
VMEM_LIMIT = 60 * 1024 * 1024


def dot(left, right, dims=PLAIN):
    return lax.dot_general(left, right, dims, preferred_element_type=jnp.float32)


def group_of(features):
    return next(size for size in (3, 2, 1) if features % size == 0)


def spread_counts(counts, step, group, feature):
    lanes = counts.shape[1]
    row = lax.broadcasted_iota(jnp.int32, (lanes, feature), 0)
    pieces = []
    for part in range(group):
        pick = (row == step * group + part).astype(jnp.float32).astype(jnp.bfloat16)
        pieces.append(dot(counts, pick))
    return pieces


def forward_b(
    slot_ref, arrived_ref, dense_ref, counts_ref, down_ref, up_ref, bias_ref,
    crossed_out, stacked_held, low_held,
):
    samples, feature = dense_ref.shape
    features = down_ref.shape[0] // feature
    group = group_of(features)
    span = group * feature
    low_held[...] = jnp.zeros_like(low_held)

    def first(step, carry):
        divisors = spread_counts(counts_ref[...], step, group, feature)
        pieces = []
        for part in range(group):
            table = jnp.maximum(step * group + part - 1, 0)
            rows = arrived_ref[slot_ref[table]].astype(jnp.float32)
            if part == 0:
                rows = jnp.where(step == 0, dense_ref[...].astype(jnp.float32), rows)
            pieces.append((rows / divisors[part]).astype(jnp.bfloat16))
        stacked = jnp.concatenate(pieces, axis=1)
        columns = pl.ds(pl.multiple_of(step * span, span), span)
        stacked_held[:, columns] = stacked
        low_held[...] += dot(stacked, down_ref[columns, :])
        return carry

    lax.fori_loop(0, features // group, first, 0)
    low = low_held[...].astype(jnp.bfloat16)

    def second(step, carry):
        columns = pl.ds(pl.multiple_of(step * span, span), span)
        projected = dot(low, up_ref[columns, :], OVER_COLS)
        wide_b = stacked_held[:, columns].astype(jnp.float32)
        crossed = wide_b * (projected + bias_ref[:, columns]) + wide_b
        crossed_out[:, columns] = crossed.astype(jnp.bfloat16)
        return carry

    lax.fori_loop(0, features // group, second, 0)


def backward_kernel(
    slot_ref, stacked_ref, upstream_ref, counts_ref, down_ref, up_ref, bias_ref,
    dense_out, slot_out, grad_down_out, grad_up_out, low_held, low_grad_held,
):
    feature = dense_out.shape[1]
    features = down_ref.shape[0] // feature
    group = group_of(features)
    span = group * feature
    low_held[...] = jnp.zeros_like(low_held)
    low_grad_held[...] = jnp.zeros_like(low_grad_held)

    def scaled(columns):
        upstream = upstream_ref[:, columns].astype(jnp.float32)
        return (upstream * stacked_ref[:, columns].astype(jnp.float32)).astype(jnp.bfloat16)

    def first(step, carry):
        columns = pl.ds(pl.multiple_of(step * span, span), span)
        low_held[...] += dot(stacked_ref[:, columns], down_ref[columns, :])
        low_grad_held[...] += dot(scaled(columns), up_ref[columns, :])
        return carry

    lax.fori_loop(0, features // group, first, 0)
    low = low_held[...].astype(jnp.bfloat16)
    low_grad = low_grad_held[...].astype(jnp.bfloat16)
    for table in range(features - 1, slot_ref.shape[0]):
        slot_out[slot_ref[table]] = jnp.zeros(slot_out.shape[1:], slot_out.dtype)

    def second(step, carry):
        columns = pl.ds(pl.multiple_of(step * span, span), span)
        grad_down_out[columns, :] = dot(
            stacked_ref[:, columns], low_grad, OVER_ROWS
        ).astype(jnp.bfloat16)
        grad_up_out[columns, :] = dot(scaled(columns), low, OVER_ROWS).astype(jnp.bfloat16)
        upstream = upstream_ref[:, columns].astype(jnp.float32)
        projected = dot(low, up_ref[columns, :], OVER_COLS)
        grad = upstream * (projected + bias_ref[:, columns]) + upstream
        grad = grad + dot(low_grad, down_ref[columns, :], OVER_COLS)
        divisors = spread_counts(counts_ref[...], step, group, feature)
        for part in range(group):
            block = grad[:, part * feature : (part + 1) * feature] / divisors[part]
            block = block.astype(jnp.bfloat16)
            number = step * group + part
            if part:
                slot_out[slot_ref[number - 1]] = block
            else:

                @pl.when(step == 0)
                def _():
                    dense_out[...] = block

                @pl.when(step > 0)
                def _():
                    slot_out[slot_ref[number - 1]] = block

        return carry

    lax.fori_loop(0, features // group, second, 0)


def backward(slot_of, stacked, upstream, counts, down, up_rows, bias, feature):
    samples, width = stacked.shape
    rank = down.shape[1]
    held = jnp.bfloat16
    vmem = pl.BlockSpec(memory_space=pltpu.VMEM)
    return pl.pallas_call(
        backward_kernel,
        out_shape=(
            jax.ShapeDtypeStruct((samples, feature), held),
            jax.ShapeDtypeStruct((slot_of.shape[0], samples, feature), held),
            jax.ShapeDtypeStruct((width, rank), held),
            jax.ShapeDtypeStruct((width, rank), held),
        ),
        in_specs=[pl.BlockSpec(memory_space=pltpu.SMEM)] + [vmem] * 6,
        out_specs=(vmem,) * 4,
        scratch_shapes=[
            pltpu.VMEM((samples, rank), jnp.float32),
            pltpu.VMEM((samples, rank), jnp.float32),
        ],
        compiler_params=pltpu.CompilerParams(vmem_limit_bytes=VMEM_LIMIT),
        cost_estimate=pl.CostEstimate(
            flops=12 * samples * width * rank, bytes_accessed=20 << 20, transcendentals=0
        ),
        name="cross_backward",
    )(slot_of, stacked, upstream, counts, down, up_rows, bias)


def divisors_of(counts):
    held = jnp.pad(counts.astype(jnp.bfloat16), ((0, 0), (1, 0)), constant_values=1)
    return jnp.pad(held, ((0, 0), (0, -held.shape[1] % 128)))


def local(
    wide,
    pooled_b,
    dense_output_second,
    counts_b,
    slot_of,
    stacked_a,
    upstream_a,
    counts_a,
    down_projection,
    proj_up,
    cross_layer_bias,
):
    feature = dense_output_second.shape[1]
    shard = down_projection.shape[0]
    rank = down_projection.shape[1]
    width = stacked_a.shape[1]
    me = lax.axis_index("wide")
    lanes = -(-shard // 128) * 128

    stacked_wide = stacked_a.astype(jnp.float32)
    upstream_wide = upstream_a.astype(jnp.float32)
    scale_grad = upstream_wide * stacked_wide
    bias_share = jnp.sum(scale_grad, axis=0).reshape(wide, shard)
    holds = (jnp.arange(wide) == me) & (lax.axis_index("pair") == 0)
    bias_own = jnp.where(holds[:, None], cross_layer_bias.astype(jnp.float32)[None, :], 0.0)
    vec = jnp.pad(jnp.concatenate([bias_share, bias_own], axis=0), ((0, 0), (0, lanes - shard)))
    down_all, up_all, vec_all, arrived = gathered(
        wide, down_projection, jnp.transpose(proj_up), vec, pooled_b
    )
    grad_bias = lax.dynamic_index_in_dim(vec_all, me, 0, keepdims=False)[:shard]
    bias = vec_all[wide:, :shard].reshape(1, width)
    down = down_all.reshape(width, rank)
    up_rows = up_all.reshape(width, rank)

    dense_gradient, slot_grad, grad_down, grad_up = backward(
        slot_of, stacked_a, upstream_a, divisors_of(counts_a), down, up_rows, bias, feature
    )
    down_sum, up_sum, returned, crossed_b = scattered(
        wide,
        grad_down.reshape(wide, shard, rank),
        grad_up.reshape(wide, shard, rank),
        slot_grad,
        (slot_of, arrived, dense_output_second, divisors_of(counts_b), down, up_rows, bias),
    )
    return (crossed_b, dense_gradient, returned, down_sum, jnp.transpose(up_sum), grad_bias)


def solution(mesh):
    return jax.shard_map(
        functools.partial(local, mesh.shape["wide"]),
        mesh=mesh,
        in_specs=(
            P("wide", None, "pair", None),
            P(("wide", "pair"), None),
            P(("wide", "pair"), None),
            P(),
            P(("wide", "pair"), None),
            P(("wide", "pair"), None),
            P(("wide", "pair"), None),
            P("wide", None),
            P(None, "wide"),
            P("wide"),
        ),
        out_specs=(
            P(("wide", "pair"), None),
            P(("wide", "pair"), None),
            P("wide", None, "pair", None),
            P("wide", None),
            P(None, "wide"),
            P("wide"),
        ),
        check_vma=False,
    )
```

```python
import functools

import jax
import jax.numpy as jnp
from jax import lax
from jax.experimental import pallas as pl
from jax.experimental.pallas import tpu as pltpu
from jax.sharding import PartitionSpec as P

MESH = pl.DeviceIdType.MESH


def flipped(index, mask):
    out = index
    bit = 1
    while bit <= mask:
        if mask & bit:
            out = out + bit - 2 * bit * lax.rem(index // bit, 2)
        bit *= 2
    return out


def stage_list(wide):
    stages = []
    mask = wide // 2
    while mask > 1:
        stages.append(("wide", mask))
        mask //= 2
    return stages + [("pair", 1), ("wide", 1)]


def meet(wide, me, pair):
    barrier = pltpu.get_barrier_semaphore()
    for offset in range(1, wide):
        pl.semaphore_signal(
            barrier, inc=1, device_id={"wide": flipped(me, offset)}, device_id_type=MESH
        )
    pl.semaphore_signal(barrier, inc=1, device_id={"pair": 1 - pair}, device_id_type=MESH)
    pl.semaphore_wait(barrier, wide)


class Exchange:
    def __init__(self, wide, me, source, target, sems):
        self.me, self.source, self.target, self.sems = me, source, target, sems
        offsets = range(wide - 1, 0, -1)
        self.plain = [offset for offset in offsets if not offset & 2]
        self.crossing = [offset for offset in offsets if offset & 2]
        self.copies = []
        self.keep = pltpu.make_async_copy(source(me), target(me), sems.at[0, 0])
        self.keep.start()

    def send(self, waiting, count):
        for offset in waiting[:count]:
            peer = flipped(self.me, offset)
            made = pltpu.make_async_remote_copy(
                src_ref=self.source(peer),
                dst_ref=self.target(self.me),
                send_sem=self.sems.at[0, offset],
                recv_sem=self.sems.at[1, offset],
                device_id={"wide": peer},
                device_id_type=MESH,
            )
            made.start()
            self.copies.append(made)
        del waiting[:count]

    def send_rest(self):
        self.send(self.plain, len(self.plain))
        self.send(self.crossing, len(self.crossing))

    def finish(self):
        self.send_rest()
        self.keep.wait()
        for made in self.copies:
            made.wait()


def gather_kernel(
    wide, down_ref, up_ref, vec_ref, pooled_ref, down_out, up_out, vec_out, arrived_out,
    vec_held, vec_got, send_sem, recv_sem, local_sem, vec_send, vec_recv, swap_sems,
):
    me = lax.axis_index("wide")
    pair = lax.axis_index("pair")
    stages = stage_list(wide)
    half = down_ref.shape[1] // 2
    starts = (pl.multiple_of(pair * half, half), pl.multiple_of((1 - pair) * half, half))
    ins, outs = (down_ref, up_ref), (down_out, up_out)

    def partner(stage):
        if stage[0] == "pair":
            return {"pair": 1 - pair}
        return {"wide": flipped(me, stage[1])}

    meet(wide, me, pair)
    sends = []

    def copy(stage, source, part, kind, received, which):
        columns = pl.ds(starts[part], half)
        block = flipped(me, source)
        if source == 0:
            src = ins[kind].at[:, columns]
        else:
            src = outs[kind].at[block, :, columns]
        return pltpu.make_async_remote_copy(
            src_ref=src,
            dst_ref=outs[kind].at[block, :, columns],
            send_sem=send_sem.at[which],
            recv_sem=recv_sem.at[received],
            device_id=partner(stage),
            device_id_type=MESH,
        )

    def slot(offset, part, kind):
        return (offset * 2 + part) * 2 + kind

    def forward(position, source, part):
        for stage in stages[position:]:
            if stage[0] == "pair":
                if part == 1 or source == 0:
                    continue
                offset, got_part = source, 1
            else:
                offset, got_part = source ^ stage[1], part
            for kind in range(2):
                made = copy(stage, source, part, kind, slot(offset, got_part, kind), len(sends))
                made.start()
                sends.append(made)

    def await_block(offset, part):
        columns = pl.ds(starts[part], half)
        block = flipped(me, offset)
        for kind in range(2):
            view = outs[kind].at[block, :, columns]
            pltpu.make_async_copy(view, view, recv_sem.at[slot(offset, part, kind)]).wait()

    def vector(index, stage):
        return pltpu.make_async_remote_copy(
            src_ref=vec_held.at[index],
            dst_ref=vec_got.at[index],
            send_sem=vec_send.at[index],
            recv_sem=vec_recv.at[index],
            device_id=partner(stage),
            device_id_type=MESH,
        )

    vec_held[0] = vec_ref[...]
    vectors = [vector(index, stage) for index, stage in enumerate(stages)]
    forward(0, 0, 0)
    forward(len(stages) - 1, 0, 1)
    vectors[0].start()
    own = []
    for kind in range(2):
        keep = pltpu.make_async_copy(ins[kind], outs[kind].at[me], local_sem.at[kind])
        keep.start()
        own.append(keep)

    each = pooled_ref.shape[0]
    swap = Exchange(
        wide,
        me,
        lambda peer: pooled_ref.at[:, peer],
        lambda owner: arrived_out.at[pl.ds(owner * each, each)],
        swap_sems,
    )
    known = [0]
    for position, stage in enumerate(stages):
        if stage[0] == "wide" and stage[1] > 2:
            swap.send(swap.plain, 2)
        else:
            swap.send_rest()
        if stage[0] == "pair":
            for offset in known[1:]:
                await_block(offset, 1)
                forward(position + 1, offset, 1)
        elif stage[1] > 1:
            arrived = [offset ^ stage[1] for offset in known]
            for offset in arrived:
                await_block(offset, 0)
                forward(position + 1, offset, 0)
            known = known + arrived
        else:
            for offset in known:
                for part in range(2):
                    await_block(offset ^ 1, part)
        vectors[position].wait_recv()
        total = vec_held[position] + vec_got[position]
        if position + 1 < len(stages):
            vec_held[position + 1] = total
            vectors[position + 1].start()
        else:
            vec_out[...] = total
    for keep in own:
        keep.wait()
    swap.finish()
    for made in sends + vectors:
        made.wait_send()


def gathered(wide, down, up, vec, pooled, collective_id=0):
    rows, rank = down.shape
    count = len(stage_list(wide))
    trees = 2 * (wide // 2 - 1 + wide // 2 - 1 + wide)
    vmem = pl.BlockSpec(memory_space=pltpu.VMEM)
    hbm = pl.BlockSpec(memory_space=pl.ANY)
    return pl.pallas_call(
        functools.partial(gather_kernel, wide),
        out_shape=(
            jax.ShapeDtypeStruct((wide, rows, rank), down.dtype),
            jax.ShapeDtypeStruct((wide, rows, rank), up.dtype),
            jax.ShapeDtypeStruct(vec.shape, vec.dtype),
            jax.ShapeDtypeStruct((pooled.shape[0] * wide,) + pooled.shape[2:], pooled.dtype),
        ),
        in_specs=[vmem, vmem, vmem, hbm],
        out_specs=(hbm, hbm, vmem, hbm),
        scratch_shapes=[
            pltpu.VMEM((count,) + vec.shape, vec.dtype),
            pltpu.VMEM((count,) + vec.shape, vec.dtype),
            pltpu.SemaphoreType.DMA((trees,)),
            pltpu.SemaphoreType.DMA((4 * wide,)),
            pltpu.SemaphoreType.DMA((2,)),
            pltpu.SemaphoreType.DMA((count,)),
            pltpu.SemaphoreType.DMA((count,)),
            pltpu.SemaphoreType.DMA((2, wide)),
        ],
        compiler_params=pltpu.CompilerParams(
            collective_id=collective_id, has_side_effects=True
        ),
        cost_estimate=pl.CostEstimate(
            flops=0, bytes_accessed=wide * rows * rank * 40, transcendentals=0
        ),
        name="weights_gather",
    )(down, up, vec, pooled)


def tree_slots(wide):
    slots = {}
    mask = 2
    while mask < wide:
        for offset in range(0, wide, 2 * mask):
            slots[(mask, offset)] = len(slots)
        mask *= 2
    return slots


def scatter_kernel(
    wide, down_ref, up_ref, slot_grad_ref, slot_ref, arrived_ref, dense_ref, counts_ref,
    weight_down_ref, weight_up_ref, bias_ref,
    down_out, up_out, returned_out, crossed_out,
    stacked_held, low_held, core_got, pair_send, pair_got, tree_send, tree_got, last_send, last_got,
    core_sems, pair_sems, tree_sems, last_sems, swap_sems,
):
    me = lax.axis_index("wide")
    pair = lax.axis_index("pair")
    stages = stage_list(wide)
    slots = tree_slots(wide)
    half = down_ref.shape[2] // 2
    mine = pl.ds(pl.multiple_of(pair * half, half), half)
    other = pl.ds(pl.multiple_of((1 - pair) * half, half), half)
    ins, outs = (down_ref, up_ref), (down_out, up_out)
    evens = list(range(0, wide, 2))
    bits = wide.bit_length()
    order = sorted(
        evens, key=lambda e: [(e >> b) & 1 for b in range(1, bits)], reverse=True
    )

    def partner(stage):
        if stage[0] == "pair":
            return {"pair": 1 - pair}
        return {"wide": flipped(me, stage[1])}

    meet(wide, me, pair)

    def remote(src, dst, sems, index, stage):
        return pltpu.make_async_remote_copy(
            src_ref=src,
            dst_ref=dst,
            send_sem=sems.at[0, index],
            recv_sem=sems.at[1, index],
            device_id=partner(stage),
            device_id_type=MESH,
        )

    core_copies = {}
    for part, columns in ((1, other), (0, mine)):
        for offset in order:
            for kind in range(2):
                made = remote(
                    ins[kind].at[flipped(me, offset ^ 1), :, columns],
                    core_got.at[kind, offset // 2, :, columns],
                    core_sems,
                    (offset // 2 * 2 + part) * 2 + kind,
                    ("wide", 1),
                )
                made.start()
                core_copies[(part, offset, kind)] = made

    each = returned_out.shape[0]
    swap = Exchange(
        wide,
        me,
        lambda peer: slot_grad_ref.at[pl.ds(peer * each, each)],
        lambda owner: returned_out.at[:, owner],
        swap_sems,
    )
    swap.send(swap.plain, wide)

    def both_cores(kind, offset, columns):
        own = ins[kind][flipped(me, offset), :, columns].astype(jnp.float32)
        return own + core_got[kind, offset // 2, :, columns].astype(jnp.float32)

    pair_copies = {}
    for offset in order:
        for kind in range(2):
            core_copies[(1, offset, kind)].wait_recv()
            pair_send[kind, offset // 2] = both_cores(kind, offset, other).astype(jnp.bfloat16)
            made = remote(
                pair_send.at[kind, offset // 2],
                pair_got.at[kind, offset // 2],
                pair_sems,
                offset // 2 * 2 + kind,
                ("pair", 1),
            )
            made.start()
            pair_copies[(offset, kind)] = made

    forward_low(
        slot_ref, arrived_ref, dense_ref, counts_ref, weight_down_ref, stacked_held, low_held
    )

    tree_copies = []
    last_copies = []
    for offset in order:
        if swap.crossing and not offset & 2:
            swap.send_rest()
        if offset == order[len(order) // 2]:
            forward_out(weight_up_ref, bias_ref, crossed_out, stacked_held, low_held)
        for kind in range(2):
            core_copies[(0, offset, kind)].wait_recv()
            pair_copies[(offset, kind)].wait_recv()
            total = both_cores(kind, offset, mine)
            total = total + pair_got[kind, offset // 2].astype(jnp.float32)
            mask = 2
            while mask < wide and not offset & mask:
                index = slots[(mask, offset)]
                view = tree_got.at[kind, index]
                pltpu.make_async_copy(view, view, tree_sems.at[1, index * 2 + kind]).wait()
                total = total + tree_got[kind, index].astype(jnp.float32)
                mask *= 2
            if mask < wide:
                index = slots[(mask, offset ^ mask)]
                tree_send[kind, index] = total.astype(jnp.bfloat16)
                made = remote(
                    tree_send.at[kind, index],
                    tree_got.at[kind, index],
                    tree_sems,
                    index * 2 + kind,
                    ("wide", mask),
                )
                made.start()
                tree_copies.append(made)
                swap.send(swap.crossing, 1)
            else:
                rounded = total.astype(jnp.bfloat16)
                last_send[kind] = rounded
                made = remote(
                    last_send.at[kind], last_got.at[kind], last_sems, kind, ("pair", 1)
                )
                made.start()
                last_copies.append(made)
                outs[kind][:, mine] = rounded.astype(jnp.float32)
    for kind in range(2):
        last_copies[kind].wait_recv()
        outs[kind][:, other] = last_got[kind].astype(jnp.float32)
    for made in list(core_copies.values()) + list(pair_copies.values()):
        made.wait_send()
    for made in tree_copies + last_copies:
        made.wait_send()
    swap.finish()


def scattered(wide, grad_down, grad_up, slot_grad, forward, collective_id=1):
    _, rows, rank = grad_down.shape
    half = rank // 2
    slots = len(tree_slots(wide))
    vmem = pl.BlockSpec(memory_space=pltpu.VMEM)
    hbm = pl.BlockSpec(memory_space=pl.ANY)
    held = jnp.bfloat16
    slots_all, samples = slot_grad.shape[:2]
    return pl.pallas_call(
        functools.partial(scatter_kernel, wide),
        out_shape=(
            jax.ShapeDtypeStruct((rows, rank), jnp.float32),
            jax.ShapeDtypeStruct((rows, rank), jnp.float32),
            jax.ShapeDtypeStruct((slots_all // wide, wide) + slot_grad.shape[1:], held),
            jax.ShapeDtypeStruct((samples, wide * rows), held),
        ),
        in_specs=[vmem, vmem, hbm, pl.BlockSpec(memory_space=pltpu.SMEM)] + [vmem] * 6,
        out_specs=(vmem, vmem, hbm, vmem),
        scratch_shapes=[
            pltpu.VMEM((samples, wide * rows), held),
            pltpu.VMEM((samples, rank), jnp.float32),
            pltpu.VMEM((2, wide // 2, rows, rank), held),
            pltpu.VMEM((2, wide // 2, rows, half), held),
            pltpu.VMEM((2, wide // 2, rows, half), held),
            pltpu.VMEM((2, slots, rows, half), held),
            pltpu.VMEM((2, slots, rows, half), held),
            pltpu.VMEM((2, rows, half), held),
            pltpu.VMEM((2, rows, half), held),
            pltpu.SemaphoreType.DMA((2, 2 * wide)),
            pltpu.SemaphoreType.DMA((2, wide)),
            pltpu.SemaphoreType.DMA((2, 2 * slots)),
            pltpu.SemaphoreType.DMA((2, 2)),
            pltpu.SemaphoreType.DMA((2, wide)),
        ],
        compiler_params=pltpu.CompilerParams(
            collective_id=collective_id, has_side_effects=True,
            vmem_limit_bytes=VMEM_LIMIT,
        ),
        cost_estimate=pl.CostEstimate(
            flops=0, bytes_accessed=wide * rows * rank * 40, transcendentals=0
        ),
        name="gradients_scatter",
    )(grad_down, grad_up, slot_grad, *forward)


OVER_ROWS = (((0,), (0,)), ((), ()))
OVER_COLS = (((1,), (1,)), ((), ()))
PLAIN = (((1,), (0,)), ((), ()))
VMEM_LIMIT = 60 * 1024 * 1024


def dot(left, right, dims=PLAIN):
    return lax.dot_general(left, right, dims, preferred_element_type=jnp.float32)


def group_of(features):
    return next(size for size in (3, 2, 1) if features % size == 0)


def spread_counts(counts, step, group, feature):
    lanes = counts.shape[1]
    row = lax.broadcasted_iota(jnp.int32, (lanes, feature), 0)
    pieces = []
    for part in range(group):
        pick = (row == step * group + part).astype(jnp.float32).astype(jnp.bfloat16)
        pieces.append(dot(counts, pick))
    return pieces


def forward_low(
    slot_ref, arrived_ref, dense_ref, counts_ref, down_ref, stacked_held, low_held
):
    samples, feature = dense_ref.shape
    features = down_ref.shape[0] // feature
    group = group_of(features)
    span = group * feature
    low_held[...] = jnp.zeros_like(low_held)

    def first(step, carry):
        divisors = spread_counts(counts_ref[...], step, group, feature)
        pieces = []
        for part in range(group):
            table = jnp.maximum(step * group + part - 1, 0)
            rows = arrived_ref[slot_ref[table]].astype(jnp.float32)
            if part == 0:
                rows = jnp.where(step == 0, dense_ref[...].astype(jnp.float32), rows)
            pieces.append((rows / divisors[part]).astype(jnp.bfloat16))
        stacked = jnp.concatenate(pieces, axis=1)
        columns = pl.ds(pl.multiple_of(step * span, span), span)
        stacked_held[:, columns] = stacked
        low_held[...] += dot(stacked, down_ref[columns, :])
        return carry

    lax.fori_loop(0, features // group, first, 0)


def forward_out(up_ref, bias_ref, crossed_out, stacked_held, low_held):
    width = up_ref.shape[0]
    span = 128 * group_of(width // 128)
    low = low_held[...].astype(jnp.bfloat16)

    def second(step, carry):
        columns = pl.ds(pl.multiple_of(step * span, span), span)
        projected = dot(low, up_ref[columns, :], OVER_COLS)
        wide_b = stacked_held[:, columns].astype(jnp.float32)
        crossed = wide_b * (projected + bias_ref[:, columns]) + wide_b
        crossed_out[:, columns] = crossed.astype(jnp.bfloat16)
        return carry

    lax.fori_loop(0, width // span, second, 0)


def backward_kernel(
    slot_ref, stacked_ref, upstream_ref, counts_ref, down_ref, up_ref, bias_ref,
    dense_out, slot_out, grad_down_out, grad_up_out, low_held, low_grad_held,
):
    feature = dense_out.shape[1]
    features = down_ref.shape[0] // feature
    group = group_of(features)
    span = group * feature
    low_held[...] = jnp.zeros_like(low_held)
    low_grad_held[...] = jnp.zeros_like(low_grad_held)

    def scaled(columns):
        upstream = upstream_ref[:, columns].astype(jnp.float32)
        return (upstream * stacked_ref[:, columns].astype(jnp.float32)).astype(jnp.bfloat16)

    def first(step, carry):
        columns = pl.ds(pl.multiple_of(step * span, span), span)
        low_held[...] += dot(stacked_ref[:, columns], down_ref[columns, :])
        low_grad_held[...] += dot(scaled(columns), up_ref[columns, :])
        return carry

    lax.fori_loop(0, features // group, first, 0)
    low = low_held[...].astype(jnp.bfloat16)
    low_grad = low_grad_held[...].astype(jnp.bfloat16)
    for table in range(features - 1, slot_ref.shape[0]):
        slot_out[slot_ref[table]] = jnp.zeros(slot_out.shape[1:], slot_out.dtype)

    def second(step, carry):
        columns = pl.ds(pl.multiple_of(step * span, span), span)
        grad_down_out[columns, :] = dot(
            stacked_ref[:, columns], low_grad, OVER_ROWS
        ).astype(jnp.bfloat16)
        grad_up_out[columns, :] = dot(scaled(columns), low, OVER_ROWS).astype(jnp.bfloat16)
        upstream = upstream_ref[:, columns].astype(jnp.float32)
        projected = dot(low, up_ref[columns, :], OVER_COLS)
        grad = upstream * (projected + bias_ref[:, columns]) + upstream
        grad = grad + dot(low_grad, down_ref[columns, :], OVER_COLS)
        divisors = spread_counts(counts_ref[...], step, group, feature)
        for part in range(group):
            block = grad[:, part * feature : (part + 1) * feature] / divisors[part]
            block = block.astype(jnp.bfloat16)
            number = step * group + part
            if part:
                slot_out[slot_ref[number - 1]] = block
            else:

                @pl.when(step == 0)
                def _():
                    dense_out[...] = block

                @pl.when(step > 0)
                def _():
                    slot_out[slot_ref[number - 1]] = block

        return carry

    lax.fori_loop(0, features // group, second, 0)


def backward(slot_of, stacked, upstream, counts, down, up_rows, bias, feature):
    samples, width = stacked.shape
    rank = down.shape[1]
    held = jnp.bfloat16
    vmem = pl.BlockSpec(memory_space=pltpu.VMEM)
    return pl.pallas_call(
        backward_kernel,
        out_shape=(
            jax.ShapeDtypeStruct((samples, feature), held),
            jax.ShapeDtypeStruct((slot_of.shape[0], samples, feature), held),
            jax.ShapeDtypeStruct((width, rank), held),
            jax.ShapeDtypeStruct((width, rank), held),
        ),
        in_specs=[pl.BlockSpec(memory_space=pltpu.SMEM)] + [vmem] * 6,
        out_specs=(vmem,) * 4,
        scratch_shapes=[
            pltpu.VMEM((samples, rank), jnp.float32),
            pltpu.VMEM((samples, rank), jnp.float32),
        ],
        compiler_params=pltpu.CompilerParams(vmem_limit_bytes=VMEM_LIMIT),
        cost_estimate=pl.CostEstimate(
            flops=12 * samples * width * rank, bytes_accessed=20 << 20, transcendentals=0
        ),
        name="cross_backward",
    )(slot_of, stacked, upstream, counts, down, up_rows, bias)


def divisors_of(counts):
    held = jnp.pad(counts.astype(jnp.bfloat16), ((0, 0), (1, 0)), constant_values=1)
    return jnp.pad(held, ((0, 0), (0, -held.shape[1] % 128)))


def local(
    wide,
    pooled_b,
    dense_output_second,
    counts_b,
    slot_of,
    stacked_a,
    upstream_a,
    counts_a,
    down_projection,
    proj_up,
    cross_layer_bias,
):
    feature = dense_output_second.shape[1]
    shard = down_projection.shape[0]
    rank = down_projection.shape[1]
    width = stacked_a.shape[1]
    me = lax.axis_index("wide")
    lanes = -(-shard // 128) * 128

    stacked_wide = stacked_a.astype(jnp.float32)
    upstream_wide = upstream_a.astype(jnp.float32)
    scale_grad = upstream_wide * stacked_wide
    bias_share = jnp.sum(scale_grad, axis=0).reshape(wide, shard)
    holds = (jnp.arange(wide) == me) & (lax.axis_index("pair") == 0)
    bias_own = jnp.where(holds[:, None], cross_layer_bias.astype(jnp.float32)[None, :], 0.0)
    vec = jnp.pad(jnp.concatenate([bias_share, bias_own], axis=0), ((0, 0), (0, lanes - shard)))
    down_all, up_all, vec_all, arrived = gathered(
        wide, down_projection, jnp.transpose(proj_up), vec, pooled_b
    )
    grad_bias = lax.dynamic_index_in_dim(vec_all, me, 0, keepdims=False)[:shard]
    bias = vec_all[wide:, :shard].reshape(1, width)
    down = down_all.reshape(width, rank)
    up_rows = up_all.reshape(width, rank)

    dense_gradient, slot_grad, grad_down, grad_up = backward(
        slot_of, stacked_a, upstream_a, divisors_of(counts_a), down, up_rows, bias, feature
    )
    down_sum, up_sum, returned, crossed_b = scattered(
        wide,
        grad_down.reshape(wide, shard, rank),
        grad_up.reshape(wide, shard, rank),
        slot_grad,
        (slot_of, arrived, dense_output_second, divisors_of(counts_b), down, up_rows, bias),
    )
    return (crossed_b, dense_gradient, returned, down_sum, jnp.transpose(up_sum), grad_bias)


def solution(mesh):
    return jax.shard_map(
        functools.partial(local, mesh.shape["wide"]),
        mesh=mesh,
        in_specs=(
            P("wide", None, "pair", None),
            P(("wide", "pair"), None),
            P(("wide", "pair"), None),
            P(),
            P(("wide", "pair"), None),
            P(("wide", "pair"), None),
            P(("wide", "pair"), None),
            P("wide", None),
            P(None, "wide"),
            P("wide"),
        ),
        out_specs=(
            P(("wide", "pair"), None),
            P(("wide", "pair"), None),
            P("wide", None, "pair", None),
            P("wide", None),
            P(None, "wide"),
            P("wide"),
        ),
        check_vma=False,
    )
```
